32 devices in a mesh: clips: 2 (over y), ha: 4 (over z), ta: 2 (over x), wa: 2 (over core).
Axes of the slice: x: 2, y: 2, z: 4, core: 2. Of those that a mesh axis runs over, the one named last changes fastest.
Arguments:
- frames: bfloat16 [8, 16, 128, 192], P(('clips', 'ta'), 'ha', 'wa'), parts along dimension 0, may hold values from -6 to 6
- cache: bfloat16 [4, 16, 128, 192], P('clips', 'ha', 'wa'), parts along dimension 0, may hold values from -5 to 5
- norm_gain: float32 [192], replicated, may hold values from 0.25 to 1.75
- conv_weight: bfloat16 [3, 3, 3, 192, 192], replicated, may hold values from -0.078125 to 0.078125
- conv_bias: float32 [192], replicated, may hold values from -3 to 3
- up_weight: bfloat16 [3, 3, 192, 96], replicated, may hold values from -0.15625 to 0.15625
- up_bias: float32 [96], replicated, may hold values from -3 to 3
Outputs:
- upsampled: bfloat16 [8, 32, 128, 192], P(('clips', 'ta'), 'ha', 'wa'), parts along dimension 0
The draws below stay inside these ranges and needn't reach their ends.
There are 2 independent parts, one for each index of `clips`. The reference program is written for one: setup_inputs(seed, part) draws one part's arguments, and reference() takes and returns one part's arrays. A program takes and returns all parts, laid end to end along the dimension named above; an argument that names none is the same for every part. Nothing has to cross between parts.
All inputs are finite; a program needn't handle non-finite values.
Results may differ from the reference program's by a relative error of at most 0.0075.
Values may be sent and summed in bfloat16 or wider, within the bound.
No kernel may reach another device: no remote copies, remote signals or barrier semaphores. Data moves between devices by JAX's collectives and lax.ppermute only.
A program may use at most 64 MiB of HBM per device.

```python
import jax
import jax.numpy as jnp
from jax import lax

C = 192
C_OUT = 96
FRAMES = 4
HEIGHT = 16
WIDTH = 128


def shard_levels(own_key, extent, split, least, top_value):
    level = 1.0
    for dim, shards_of in split:
        draws = jax.random.uniform(jax.random.fold_in(jax.random.fold_in(own_key, 6), dim), (shards_of,), jnp.float32, least / len(split), top_value / len(split))
        level = level * jnp.repeat(jnp.exp(draws), extent[dim] // shards_of).reshape((-1,) + (1,) * (len(extent) - 1 - dim))
    return level


def normal_values(stream_key, dims, spread, limit, shards=(), kind=jnp.bfloat16):
    drawn = spread * jax.random.normal(stream_key, dims, jnp.float32)
    if shards:
        drawn = drawn * shard_levels(stream_key, dims, shards, -0.22, 0.18)
    return jnp.clip(drawn, -limit, limit).astype(kind)


def setup_inputs(seed: int = 0, part: int = 0) -> dict:
    key_list = jax.random.split(jax.random.key(seed), 8)
    part_splits = jax.random.split(jax.random.fold_in(key_list[7], part), 8)
    return {
        "frames": normal_values(part_splits[0], (FRAMES, HEIGHT, WIDTH, C), 1.0, 6.0, ((0, 2), (1, 4), (2, 2))),
        "cache": normal_values(part_splits[1], (2, HEIGHT, WIDTH, C), 0.7, 5.0, ((1, 4), (2, 2))),
        "norm_gain": jnp.clip(1.0 + 0.15 * jax.random.normal(key_list[2], (C,), jnp.float32), 0.25, 1.75),
        "conv_weight": normal_values(key_list[3], (3, 3, 3, C, C), (27 * C) ** -0.5, 0.078125),
        "conv_bias": normal_values(key_list[4], (C,), 0.5, 3.0, (), jnp.float32),
        "up_weight": normal_values(key_list[5], (3, 3, C, C_OUT), (9 * C) ** -0.5, 0.15625),
        "up_bias": normal_values(key_list[6], (C_OUT,), 0.5, 3.0, (), jnp.float32),
    }


EPS = 1e-06

def activate(values, gain):
    wide = values.astype(jnp.float32)
    scale = lax.rsqrt(lax.optimization_barrier(jnp.mean(wide * wide, axis=-1, keepdims=True)) + EPS)
    return jax.nn.silu(wide * scale * gain).astype(jnp.bfloat16)

def causal_conv(padded, weight, count, rows, cols):
    channels = padded.shape[-1]
    total = jnp.zeros((count * rows * cols, weight.shape[-1]), jnp.float32)
    for a in range(3):
        for b in range(3):
            for c in range(3):
                window = padded[a:a + count, b:b + rows, c:c + cols].reshape(-1, channels)
                total = total + jnp.dot(window, weight[a, b, c], preferred_element_type=jnp.float32)
    return total.reshape(count, rows, cols, -1)

def upsample_conv(bordered, weight, bias):
    doubled = jnp.repeat(jnp.repeat(bordered, 2, axis=1), 2, axis=2)[:, 1:-1, 1:-1]
    count = doubled.shape[0]
    rows = doubled.shape[1] - 2
    cols = doubled.shape[2] - 2
    channels = doubled.shape[-1]
    total = jnp.zeros((count * rows * cols, weight.shape[-1]), jnp.float32)
    for a in range(3):
        for b in range(3):
            window = doubled[:, a:a + rows, b:b + cols].reshape(-1, channels)
            total = total + jnp.dot(window, weight[a, b], preferred_element_type=jnp.float32)
    result = (total + bias).astype(jnp.bfloat16)
    return result.reshape(count, rows, cols // 2, 2 * weight.shape[-1])

def reference(frames, cache, norm_gain, conv_weight, conv_bias, up_weight, up_bias):
    count, rows, cols, channels = frames.shape
    activated = activate(frames, norm_gain)
    extended = jnp.concatenate([cache, activated], axis=0)
    padded = jnp.pad(extended, ((0, 0), (1, 1), (1, 1), (0, 0)))
    convolved = causal_conv(padded, conv_weight, count, rows, cols)
    residual = (frames.astype(jnp.float32) + convolved + conv_bias).astype(jnp.bfloat16)
    bordered = jnp.pad(residual, ((0, 0), (1, 1), (1, 1), (0, 0)))
    return upsample_conv(bordered, up_weight, up_bias)
```

```python
import functools

import jax
import jax.numpy as jnp
from jax import lax
from jax.experimental import pallas as pl
from jax.experimental.pallas import tpu as pltpu
from jax.sharding import PartitionSpec as P


EPS = 1e-06
HALO = 2
LANES = 128
BLOCK = 16
SUBLANES = 8
AXES = ("ha", "ta", "wa")


def ring(axis):
    count = lax.axis_size(axis)
    return [(i, (i + 1) % count) for i in range(count)]


def snake(towards, later):
    chips, steps, cores = (lax.axis_size(axis) for axis in AXES)
    pairs = []
    for h in range(chips):
        for t in range(steps):
            for w in range(cores):
                step, target, core = (t + later) % steps, h + towards[w], w
                if not 0 <= target < chips:
                    target, core = h, cores - 1 - w
                pairs.append(((h * steps + t) * cores + w, (target * steps + step) * cores + core))
    return pairs


def activate(values, gain):
    wide = values.astype(jnp.float32)
    scale = lax.rsqrt(jnp.sum(wide * wide, axis=-1, keepdims=True) / wide.shape[-1] + EPS)
    v = wide * scale * gain
    return v / (1.0 + jnp.exp(-v))


def packed(cells):
    rest = jnp.concatenate([cells[0, :, :, LANES:], cells[1, :, :, LANES:]], axis=-1)
    return jnp.stack([cells[0, :, :, :LANES], cells[1, :, :, :LANES], rest])


def fetch(sources, targets, arrived):
    copies = [pltpu.make_async_copy(*pair, arrived.at[i]) for i, pair in enumerate(zip(sources, targets))]
    for copy in copies:
        copy.start()
    return copies


def pack_kernel(frames_hbm, cache_hbm, gain_hbm, first, second, raw_first, raw_second, act,
                frames, cache, gain, arrived):
    left = lax.axis_index("wa") == 0
    last = lax.axis_index("ta") == lax.axis_size("ta") - 1
    for copy in fetch((gain_hbm, frames_hbm, cache_hbm), (gain, frames, cache), arrived):
        copy.wait()
    cells = frames[...]
    active = activate(cells, gain[...].reshape(1, -1)).astype(jnp.bfloat16)
    act[...] = active
    sent = packed(jnp.where(last, cache[...], active))
    first[...] = jnp.where(left, sent[:, :HALO], sent[:, HALO:])
    second[...] = jnp.where(left, sent[:, HALO:], sent[:, :HALO])
    sent = packed(cells)
    raw_first[...] = jnp.where(left, sent[:, HALO:], sent[:, :HALO])
    raw_second[...] = jnp.where(left, sent[:, :HALO], sent[:, HALO:])


def prep_kernel(conv_hbm, up_hbm, gain_hbm, bias_hbm, up_bias_hbm, conv, folded, lines,
                weight, gain, bias, up_bias, arrived):
    copies = fetch((gain_hbm, bias_hbm, up_bias_hbm, up_hbm, conv_hbm), (gain, bias, up_bias, weight, conv), arrived)
    for copy in copies[:-1]:
        copy.wait()
    taps = [[weight[a, b].astype(jnp.float32) for b in range(3)] for a in range(3)]
    columns = []
    for rows in ((0,), (1, 2), (0, 1), (2,)):
        columns.append([functools.reduce(jnp.add, [taps[a][b] for a in rows]) for b in range(3)])
    for i, (one, two, three) in enumerate(columns):
        folded[2 * i] = jnp.concatenate([two + three, one + two], axis=-1).astype(jnp.bfloat16)
        folded[2 * i + 1] = jnp.concatenate([one, three], axis=-1).astype(jnp.bfloat16)
    line = up_bias[...].reshape(1, -1)
    for i, value in enumerate((gain[...].reshape(1, -1), bias[...].reshape(1, -1), jnp.concatenate([line, line], axis=-1))):
        lines[i] = jnp.broadcast_to(value, lines.shape[1:])
    copies[-1].wait()


def unpack(planes, cells, start):
    rows = planes.shape[1]
    rest = cells.shape[-1] - LANES
    for f in range(2):
        cells[f, pl.ds(start, rows), :, :LANES] = planes[f, :, :, :]
        cells[f, pl.ds(start, rows), :, LANES:] = planes[2, :, :, f * rest : (f + 1) * rest]


def edge_columns(near, edges, left):
    frames, rows = near.shape[0], near.shape[1]
    for f in range(frames):
        for r in range(rows):
            block = near[f, r].astype(jnp.float32)
            for s in range(HALO):
                line = jnp.where(left, block[s : s + 1], block[BLOCK - 1 - s : BLOCK - s])
                edges[f, s * rows + r : s * rows + r + 1, :] = line
        edges[f, HALO * rows :, :] = jnp.zeros((SUBLANES, near.shape[-1]), jnp.float32)


def conv_sums(cells, edges, weight, taps, rows):
    channels = cells.shape[-1]
    cols = cells.shape[2]
    sums = [None, None, None]
    for a, f in taps:
        for b in range(3):
            side = jnp.concatenate(
                [edges[f, b : b + SUBLANES], edges[f, SUBLANES + b : 2 * SUBLANES + b]], axis=0
            ).astype(jnp.bfloat16)
            window = jnp.concatenate(
                [cells[f, b : b + rows].reshape(rows * cols, channels), side], axis=0
            )
            for c in range(3):
                part = jnp.dot(window, weight[a, b, c], preferred_element_type=jnp.float32)
                sums[c] = part if sums[c] is None else sums[c] + part
    return sums


def shifted_sum(sums, before, after, rows, cols, left):
    channels = sums[0].shape[-1]
    size = rows * cols
    lo, hi = SUBLANES, SUBLANES + cols
    side = [total[size:] for total in sums]
    before[:, lo:hi, :] = sums[0][:size].reshape(rows, cols, channels)
    after[:, lo:hi, :] = sums[2][:size].reshape(rows, cols, channels)
    zero = jnp.zeros((1, channels), jnp.float32)
    for r in range(rows):
        before[r, lo - 1 : lo, :] = jnp.where(left, zero, side[0][r : r + 1])
        after[r, hi : hi + 1, :] = jnp.where(left, side[2][r : r + 1], zero)
    body = sums[1][:size].reshape(rows, cols, channels)
    body = body + before[:, lo - 1 : hi - 1, :] + after[:, lo + 1 : hi + 1, :]
    pad = jnp.zeros((SUBLANES - rows, channels), jnp.float32)
    inner = [jnp.concatenate([before[r, hi - 1 : hi, :] for r in range(rows)] + [pad], axis=0),
             jnp.concatenate([after[r, lo : lo + 1, :] for r in range(rows)] + [pad], axis=0)]
    outer = [side[0][SUBLANES:], side[2][SUBLANES:]]
    edge = side[1][:SUBLANES] + jnp.where(left, inner[0] + outer[1], outer[0] + inner[1])
    return body, edge


def place():
    chip = lax.axis_index("ha")
    core = lax.axis_index("wa")
    return core == 0, core, chip == 0, chip == lax.axis_size("ha") - 1


def row_valid(count, top, bottom, halo):
    row = lax.broadcasted_iota(jnp.int32, (count, 1), 0) % SUBLANES
    rows = SUBLANES if halo == HALO else SUBLANES - 2 * (HALO - halo)
    outside = (top & (row < halo)) | (bottom & (row >= rows - halo))
    return jnp.logical_not(outside)


def own_kernel(frames_hbm, act, top_a, top_b, sib, sib_ends, weight, lines, body_out, edge_out,
               frames, raw, cells, near, edges, live, before, after, arrived):
    copies = fetch((frames_hbm,), (frames,), arrived)
    left, core, top, bottom = place()
    count, rows, cols, channels = frames.shape
    gains, biases = lines[0, :1], lines[1, :1]
    far = rows + HALO
    upper, lower = core * far, (1 - core) * far
    unpack(top_a, raw, upper)
    unpack(top_b, raw, lower)
    cells[:, HALO:far] = act[...]
    for start, outside in ((0, top), (far, bottom)):
        value = activate(raw[:, start : start + HALO], gains).astype(jnp.bfloat16)
        cells[:, start : start + HALO] = jnp.where(outside, jnp.zeros_like(value), value)
    offset = pl.multiple_of(core * (cols - BLOCK), BLOCK)
    near[:, HALO:far] = sib[:, :, pl.ds(offset, BLOCK), :]
    unpack(sib_ends[:, :HALO], near, lower)
    unpack(sib_ends[:, HALO:], near, upper)
    edge_columns(near, edges, left)
    inside = row_valid(2 * SUBLANES, top, bottom, HALO)
    for f in range(count):
        value = activate(edges[f, : 2 * SUBLANES], gains)
        live[f, : 2 * SUBLANES] = jnp.where(inside, value, jnp.zeros_like(value))
        live[f, 2 * SUBLANES :] = jnp.zeros((SUBLANES, channels), jnp.float32)
    mid = rows + 2
    copies[0].wait()
    raw[:, HALO:far] = frames[...]
    for t in range(count):
        taps = [(a, t + a - 2) for a in range(3) if 0 <= t + a - 2]
        sums = conv_sums(cells, live, weight, taps, mid)
        body, edge = shifted_sum(sums, before, after, mid, cols, left)
        body_out[t] = body + raw[t, 1 : 1 + mid].astype(jnp.float32) + biases
        edge_out[t] = edge + edges[t, 1 : 1 + SUBLANES] + biases


def rest_kernel(main_a, main_b, top_a, top_b, sib, weight, body_in, edge_in, folded, lines, out,
                cells, near, edges, before, after, res, rim, wide):
    left, core, top, bottom = place()
    count, mid, cols, channels = body_in.shape
    rows = mid - 2
    far = rows + HALO
    unpack(main_a, cells, HALO + core * HALO)
    unpack(main_b, cells, HALO + (1 - core) * HALO)
    unpack(top_a, cells, core * far)
    unpack(top_b, cells, (1 - core) * far)
    zero = jnp.zeros((2, HALO, cols, channels), jnp.bfloat16)
    cells[:, :HALO] = jnp.where(top, zero, cells[:, :HALO])
    cells[:, far:] = jnp.where(bottom, zero, cells[:, far:])
    starts = (HALO + (1 - core) * HALO, HALO + core * HALO, (1 - core) * far, core * far)
    for i, start in enumerate(starts):
        unpack(sib[:, i * HALO : (i + 1) * HALO], near, start)
    edge_columns(near, edges, left)
    inside = row_valid(2 * SUBLANES, top, bottom, HALO)
    for f in range(2):
        value = edges[f, : 2 * SUBLANES]
        edges[f, : 2 * SUBLANES] = jnp.where(inside, value, jnp.zeros_like(value))
    ring_inside = row_valid(SUBLANES, top, bottom, 1)
    line = jnp.zeros((cols, channels), jnp.bfloat16)
    for t in range(count):
        taps = [(a, t + a) for a in range(3) if t + a < 2]
        if taps:
            sums = conv_sums(cells, edges, weight, taps, mid)
            body, edge = shifted_sum(sums, before, after, mid, cols, left)
            body, edge = body + body_in[t], edge + edge_in[t]
        else:
            body, edge = body_in[t], edge_in[t]
        body = body.astype(jnp.bfloat16)
        res[t] = body
        res[t, 0] = jnp.where(top, line, body[0])
        res[t, mid - 1] = jnp.where(bottom, line, body[mid - 1])
        rim[t, :SUBLANES] = jnp.where(ring_inside, edge, jnp.zeros_like(edge))
        rim[t, SUBLANES:] = jnp.zeros((SUBLANES, channels), jnp.float32)
    size = count * rows * cols
    lo, hi = SUBLANES, SUBLANES + cols
    lane = lax.broadcasted_iota(jnp.int32, (1, 1, channels), 2)
    early = lane < channels // 2
    nothing = jnp.zeros((1, channels), jnp.float32)
    windows = []
    for k in range(3):
        window = [res[t, k : k + rows].reshape(rows * cols, channels) for t in range(count)]
        window += [
            jnp.concatenate([rim[t, k : k + SUBLANES] for t in range(count)], axis=0).astype(jnp.bfloat16)
        ]
        windows.append(jnp.concatenate(window, axis=0))
    for p in range(2):
        centre = sides = None
        for k in range(2):
            i = 2 * (2 * p + k)
            one = jnp.dot(windows[p + k], folded[i], preferred_element_type=jnp.float32)
            two = jnp.dot(windows[p + k], folded[i + 1], preferred_element_type=jnp.float32)
            centre = one if centre is None else centre + one
            sides = two if sides is None else sides + two
        wide[:, lo:hi, :] = sides[:size].reshape(count * rows, cols, channels)
        for t in range(count):
            for r in range(rows):
                value = sides[size + t * SUBLANES + r : size + t * SUBLANES + r + 1]
                wide[t * rows + r, lo - 1 : lo, :] = jnp.where(left, nothing, value)
                wide[t * rows + r, hi : hi + 1, :] = jnp.where(left, value, nothing)
        total = centre[:size].reshape(count * rows, cols, channels)
        total = total + jnp.where(early, wide[:, lo - 1 : hi - 1, :], wide[:, lo + 1 : hi + 1, :])
        total = (total + lines[2, :1].reshape(1, 1, -1)).astype(jnp.bfloat16)
        for t in range(count):
            for r in range(rows):
                out[t, 2 * r + p] = total[t * rows + r]


VMEM = pl.BlockSpec(memory_space=pltpu.VMEM)
HBM = pl.BlockSpec(memory_space=pltpu.HBM)


def call(kernel, specs, shapes, scratch, flops, *args):
    return pl.pallas_call(
        kernel,
        out_shape=shapes,
        in_specs=specs,
        out_specs=jax.tree.map(lambda _: VMEM, shapes),
        scratch_shapes=scratch,
        cost_estimate=pl.CostEstimate(flops=flops, transcendentals=0, bytes_accessed=0),
        compiler_params=pltpu.CompilerParams(vmem_limit_bytes=40 * 1024 * 1024),
    )(*[pltpu.with_memory_space_constraint(arg, pltpu.HBM) if spec is HBM else arg for spec, arg in zip(specs, args)])


def near_sibling(parts):
    start = (1 - lax.axis_index("wa")) * (parts[0].shape[2] - BLOCK)
    return jnp.concatenate([lax.dynamic_slice_in_dim(part, start, BLOCK, axis=2) for part in parts], axis=1)


def block(frames, cache, norm_gain, conv_weight, conv_bias, up_weight, up_bias):
    count, rows, cols, channels = frames.shape
    outputs = up_weight.shape[-1]
    cores = lax.axis_size("wa")
    f32, bf16 = jnp.float32, jnp.bfloat16
    shape = jax.ShapeDtypeStruct
    part = shape((3, HALO, cols, LANES), bf16)
    sibling = [(i, cores - 1 - i) for i in range(cores)]
    along, against, later = snake((1, -1), 0), snake((-1, 1), 0), snake((1, -1), 1)
    sib = lax.ppermute(frames, "wa", sibling)
    first, second, raw_first, raw_second, act = call(
        pack_kernel, [HBM] * 3, (part, part, part, part, shape(frames.shape, bf16)),
        (pltpu.VMEM(frames.shape, bf16), pltpu.VMEM(cache.shape, bf16), pltpu.VMEM(norm_gain.shape, f32),
         pltpu.SemaphoreType.DMA((3,))),
        0, frames, cache, norm_gain,
    )
    main_a = lax.ppermute(first, "ta", ring("ta"))
    main_b = lax.ppermute(second, "ta", ring("ta"))
    prev_a = lax.ppermute(second, AXES, later)
    own_a = lax.ppermute(raw_first, AXES, along)
    own_b = lax.ppermute(raw_second, AXES, against)
    prev_b = lax.ppermute(main_a, AXES, against)
    sib_own = lax.ppermute(near_sibling([own_a, own_b]), "wa", sibling)
    sib_prev = lax.ppermute(near_sibling([main_a, main_b, prev_a, prev_b]), "wa", sibling)
    weight, folded, lines = call(
        prep_kernel, [HBM] * 5,
        (shape(conv_weight.shape, bf16), shape((8, channels, 2 * outputs), bf16), shape((3, SUBLANES, channels), f32)),
        (pltpu.VMEM(up_weight.shape, bf16), pltpu.VMEM(norm_gain.shape, f32), pltpu.VMEM(conv_bias.shape, f32),
         pltpu.VMEM(up_bias.shape, f32), pltpu.SemaphoreType.DMA((5,))),
        10**9, conv_weight, up_weight, norm_gain, conv_bias, up_bias,
    )
    mid, all_rows = rows + 2, rows + 2 * HALO
    grid = pltpu.VMEM((count, all_rows, cols, channels), bf16)
    near = pltpu.VMEM((count, all_rows, BLOCK, channels), bf16)
    edges = pltpu.VMEM((count, 3 * SUBLANES, channels), f32)
    shift = pltpu.VMEM((mid, cols + 2 * SUBLANES, channels), f32)
    body, edge = call(
        own_kernel, [HBM] + [VMEM] * 7,
        (shape((count, mid, cols, channels), f32), shape((count, SUBLANES, channels), f32)),
        (pltpu.VMEM(frames.shape, bf16), grid, grid, near, edges, edges, shift, shift, pltpu.SemaphoreType.DMA((1,))),
        10**9, frames, act, own_a, own_b, sib, sib_own, weight, lines,
    )
    return call(
        rest_kernel, [VMEM] * 10, shape((count, 2 * rows, cols, 2 * outputs), bf16),
        (grid, near, edges, shift, shift,
         pltpu.VMEM((count, mid, cols, channels), bf16), pltpu.VMEM((count, 2 * SUBLANES, channels), f32),
         pltpu.VMEM((count * rows, cols + 2 * SUBLANES, channels), f32)), 10**9,
        main_a, main_b, prev_a, prev_b, sib_prev, weight, body, edge, folded, lines,
    )


def solution(mesh):
    return jax.shard_map(
        block,
        mesh=mesh,
        in_specs=(
            P(("clips", "ta"), "ha", "wa", None),
            P("clips", "ha", "wa", None),
            P(),
            P(),
            P(),
            P(),
            P(),
        ),
        out_specs=P(("clips", "ta"), "ha", "wa", None),
        check_vma=False,
    )
```

```python
import functools

import jax
import jax.numpy as jnp
from jax import lax
from jax.experimental import pallas as pl
from jax.experimental.pallas import tpu as pltpu
from jax.sharding import PartitionSpec as P


EPS = 1e-06
HALO = 2
LANES = 128
COST = 10**9
BLOCK = 8
SUBLANES = 8
AXES = ("ha", "ta", "wa")


def ring(axis):
    count = lax.axis_size(axis)
    return [(i, (i + 1) % count) for i in range(count)]


def snake(towards, later):
    chips, steps, cores = (lax.axis_size(axis) for axis in AXES)
    pairs = []
    for h in range(chips):
        for t in range(steps):
            for w in range(cores):
                step, target, core = (t + later) % steps, h + towards[w], w
                if not 0 <= target < chips:
                    target, core = h, cores - 1 - w
                pairs.append(((h * steps + t) * cores + w, (target * steps + step) * cores + core))
    return pairs


def activate(values, gain):
    wide = values.astype(jnp.float32)
    scale = lax.rsqrt(jnp.sum(wide * wide, axis=-1, keepdims=True) / wide.shape[-1] + EPS)
    v = wide * scale * gain
    return v / (1.0 + jnp.exp(-v))


def packed(cells):
    rest = jnp.concatenate([cells[0, :, :, LANES:], cells[1, :, :, LANES:]], axis=-1)
    return jnp.stack([cells[0, :, :, :LANES], cells[1, :, :, :LANES], rest])


def fetch(sources, targets, arrived):
    copies = [pltpu.make_async_copy(*pair, arrived.at[i]) for i, pair in enumerate(zip(sources, targets))]
    for copy in copies:
        copy.start()
    return copies


def pack_kernel(frames_hbm, cache_hbm, gain_hbm, first, second, raw_first, raw_second, act,
                frames, cache, gain, arrived):
    left = lax.axis_index("wa") == 0
    last = lax.axis_index("ta") == lax.axis_size("ta") - 1
    copies = fetch((gain_hbm, frames_hbm, cache_hbm), (gain, frames, cache), arrived)
    for copy in copies[:2]:
        copy.wait()
    cells = frames[...]
    active = activate(cells, gain[...].reshape(1, -1)).astype(jnp.bfloat16)
    act[...] = active
    copies[2].wait()
    sent = packed(jnp.where(last, cache[...], active))
    first[...] = jnp.where(left, sent[:, :HALO], sent[:, HALO:])
    second[...] = jnp.where(left, sent[:, HALO:], sent[:, :HALO])
    sent = packed(cells)
    raw_first[...] = jnp.where(left, sent[:, HALO:], sent[:, :HALO])
    raw_second[...] = jnp.where(left, sent[:, :HALO], sent[:, HALO:])


def place():
    chip = lax.axis_index("ha")
    core = lax.axis_index("wa")
    return core == 0, core, chip == 0, chip == lax.axis_size("ha") - 1


def unpack(planes, cells, start):
    rows = planes.shape[1]
    rest = cells.shape[-1] - LANES
    for f in range(2):
        cells[f, pl.ds(start, rows), :, :LANES] = planes[f, :, :, :]
        cells[f, pl.ds(start, rows), :, LANES:] = planes[2, :, :, f * rest : (f + 1) * rest]


def clear_outside(cells, top, bottom):
    zero = jnp.zeros((2, HALO) + cells.shape[2:], cells.dtype)
    cells[:, :HALO] = jnp.where(top, zero, cells[:, :HALO])
    cells[:, HALO:] = jnp.where(bottom, zero, cells[:, HALO:])


def row_sums(inner, outer, weight, c, mid):
    parts = [[] for _ in range(mid)]
    for b in range(3):
        if inner:
            rows, cols, channels = inner[0][1].shape
            total = None
            for a, cells in inner:
                part = jnp.dot(cells.reshape(rows * cols, channels), weight[a, b, c], preferred_element_type=jnp.float32)
                total = part if total is None else total + part
            for r in range(rows):
                parts[r + HALO - b].append(total[r * cols : (r + 1) * cols])
        if outer:
            cols, channels = outer[0][1].shape[1:]
            total = None
            for a, cells in outer:
                window = cells[b : b + HALO].reshape(HALO * cols, channels)
                part = jnp.dot(window, weight[a, b, c], preferred_element_type=jnp.float32)
                total = part if total is None else total + part
            for r, target in enumerate(((0, 1), (0, mid - 1), (mid - 2, mid - 1))[b]):
                parts[target].append(total[r * cols : (r + 1) * cols])
    return [functools.reduce(jnp.add, part) if part else None for part in parts]


def add_taps(inner, outer, weight, base, rim, before, after, left):
    mid = len(base)
    channels = weight.shape[-1]
    lo, hi = SUBLANES, before.shape[1] - SUBLANES
    zero = jnp.zeros((1, channels), jnp.float32)
    first, second, third = [row_sums(inner, outer, weight, c, mid) for c in range(3)]
    total, line = [], []
    for r in range(mid):
        if second[r] is None:
            total.append(base[r])
            line.append(zero)
            continue
        before[r, lo - 1 : lo, :] = zero
        after[r, hi : hi + 1, :] = zero
        before[r, lo:hi, :] = first[r]
        after[r, lo:hi, :] = third[r]
        value = second[r] + before[r, lo - 1 : hi - 1, :] + after[r, lo + 1 : hi + 1, :]
        total.append(value if base[r] is None else base[r] + value)
        line.append(jnp.where(left, before[r, hi - 1 : hi, :], after[r, lo : lo + 1, :]))
    line = jnp.concatenate(line + [zero] * (SUBLANES - mid), axis=0)
    return total, line if rim is None else rim + line


def first_kernel(raw_first, raw_second, act, weight, bias, body_out, edge_out, frames, before, after):
    left, core, _, _ = place()
    count, mid, cols, channels = body_out.shape
    unpack(raw_first, frames, (1 - core) * HALO)
    unpack(raw_second, frames, core * HALO)
    line = bias[...].reshape(1, -1)
    none = jnp.broadcast_to(line, (cols, channels))
    for t in range(count):
        inner = [(a, act[t + a - 2]) for a in range(3) if 0 <= t + a - 2]
        base = [none] + [frames[t, r].astype(jnp.float32) + line for r in range(mid - 2)] + [none]
        total, edge = add_taps(inner, [], weight, base, None, before, after, left)
        for r in range(mid):
            body_out[t, r] = total[r]
        edge_out[t] = edge


def second_kernel(main_a, main_b, own_a, own_b, weight, gain, body_in, edge_in, body_out, edge_out,
                  main, raw, halo, before, after):
    left, core, top, bottom = place()
    count, mid, _, _ = body_in.shape
    unpack(main_a, main, core * HALO)
    unpack(main_b, main, (1 - core) * HALO)
    unpack(own_a, raw, core * HALO)
    unpack(own_b, raw, (1 - core) * HALO)
    halo[...] = activate(raw[...], gain[...].reshape(1, -1)).astype(jnp.bfloat16)
    clear_outside(halo, top, bottom)
    for t in range(count):
        inner = [(a, main[t + a]) for a in range(3) if t + a < 2]
        outer = [(a, halo.at[t + a - 2]) for a in range(3) if 0 <= t + a - 2]
        base = [body_in[t, r] for r in range(mid)]
        base[0] = base[0] + raw[t, HALO - 1].astype(jnp.float32)
        base[-1] = base[-1] + raw[t, HALO].astype(jnp.float32)
        total, edge = add_taps(inner, outer, weight, base, edge_in[t], before, after, left)
        for r in range(mid):
            body_out[t, r] = total[r]
        edge_out[t] = edge


def fold_kernel(weight, folded):
    taps = [[weight[a, b].astype(jnp.float32) for b in range(3)] for a in range(3)]
    columns = []
    for rows in ((0,), (1, 2), (0, 1), (2,)):
        columns.append([functools.reduce(jnp.add, [taps[a][b] for a in rows]) for b in range(3)])
    for i, (one, two, three) in enumerate(columns):
        folded[2 * i] = jnp.concatenate([two + three, one + two], axis=-1).astype(jnp.bfloat16)
        folded[2 * i + 1] = jnp.concatenate([one, three], axis=-1).astype(jnp.bfloat16)


def phase_sums(windows, folded, p):
    centre = sides = None
    for k in range(2):
        i = 2 * (2 * p + k)
        one = jnp.dot(windows[p + k], folded[i], preferred_element_type=jnp.float32)
        two = jnp.dot(windows[p + k], folded[i + 1], preferred_element_type=jnp.float32)
        centre = one if centre is None else centre + one
        sides = two if sides is None else sides + two
    return centre, sides


def phase_lines(bias, channels):
    line = bias[...].reshape(1, -1)
    early = lax.broadcasted_iota(jnp.int32, (1, channels), 1) < channels // 2
    return jnp.concatenate([line, line], axis=-1), early


def third_kernel(prev_a, prev_b, weight, folded, up_bias, body_in, edge_in, block_out, edge_out, out,
                 halo, before, after, res, wide):
    left, core, top, bottom = place()
    count, mid, cols, channels = body_in.shape
    unpack(prev_a, halo, core * HALO)
    unpack(prev_b, halo, (1 - core) * HALO)
    clear_outside(halo, top, bottom)
    for t in range(count):
        outer = [(a, halo.at[t + a]) for a in range(3) if t + a < 2]
        base = [body_in[t, r] for r in range(mid)]
        total, line = add_taps([], outer, weight, base, edge_in[t], before, after, left)
        edge_out[t] = line
        for r in range(mid):
            block_out[t, r] = jnp.where(left, total[r][cols - BLOCK :], total[r][:BLOCK])
            value = total[r].astype(jnp.bfloat16)
            if r in (0, mid - 1):
                value = jnp.where(bottom if r else top, jnp.zeros_like(value), value)
            res[t, r] = value
    rows = mid - 2
    lo, hi = SUBLANES, SUBLANES + cols
    line, early = phase_lines(up_bias, channels)
    nothing = jnp.zeros((1, channels), jnp.float32)
    for t in range(count):
        windows = [res[t, k : k + rows].reshape(rows * cols, channels) for k in range(3)]
        for p in range(2):
            centre, sides = phase_sums(windows, folded, p)
            for r in range(rows):
                wide[p, r, lo:hi, :] = sides[r * cols : (r + 1) * cols]
                wide[p, r, lo - 1 : lo, :] = nothing
                wide[p, r, hi : hi + 1, :] = nothing
                total = centre[r * cols : (r + 1) * cols]
                total = total + jnp.where(early, wide[p, r, lo - 1 : hi - 1, :], wide[p, r, lo + 1 : hi + 1, :])
                out[t, 2 * r + p] = (total + line).astype(jnp.bfloat16)


def edge_columns(near, edges, left):
    frames, rows = near.shape[0], near.shape[1]
    for f in range(frames):
        for r in range(rows):
            block = near[f, r].astype(jnp.float32)
            for s in range(HALO):
                line = jnp.where(left, block[s : s + 1], block[BLOCK - 1 - s : BLOCK - s])
                edges[f, s * rows + r : s * rows + r + 1, :] = line
        edges[f, HALO * rows :, :] = jnp.zeros((SUBLANES, near.shape[-1]), jnp.float32)


def near_kernel(*refs):
    left = lax.axis_index("wa") == 0
    out, start = refs[-1], 0
    for part in refs[:-1]:
        rows, cols = part.shape[1:3]
        out[:, start : start + rows] = jnp.where(left, part[:, :, cols - BLOCK :, :], part[:, :, :BLOCK, :])
        start += rows


def row_valid(count, rows, top, bottom, halo):
    row = lax.broadcasted_iota(jnp.int32, (count, 1), 0) % SUBLANES
    return jnp.logical_not((top & (row < halo)) | (bottom & (row >= rows - halo)))


def last_kernel(sib, weight, block_in, edge_in, folded, gain, bias, up_bias, done, out_hbm,
                near_prev, near_own, edges, raw, wide, block, sent):
    left, core, top, bottom = place()
    count, mid, _, channels = block_in.shape
    rows = mid - 2
    cols = done.shape[2]
    far = rows + HALO
    rest = pl.ds(pl.multiple_of(core * BLOCK, BLOCK), cols - BLOCK)
    strip = pl.ds(pl.multiple_of((1 - core) * (cols - BLOCK), BLOCK), BLOCK)
    copies = [
        pltpu.make_async_copy(done.at[t, :, rest, :], out_hbm.at[t, :, rest, :], sent.at[t]) for t in range(count)
    ]
    for copy in copies:
        copy.start()
    starts = (HALO + (1 - core) * HALO, HALO + core * HALO, (1 - core) * far, core * far)
    for i, start in enumerate(starts):
        unpack(sib[:, i * HALO : (i + 1) * HALO], near_prev, start)
    starts = ((1 - core) * far, core * far, HALO + core * HALO, HALO + (1 - core) * HALO)
    for i, start in enumerate(starts):
        unpack(sib[:, 4 * HALO + i * HALO : 4 * HALO + (i + 1) * HALO], near_own, start)
    edge_columns(near_prev, edges.at[:2], left)
    edge_columns(near_own, raw, left)
    inside = row_valid(2 * SUBLANES, SUBLANES, top, bottom, HALO)
    for f in range(2 + count):
        value = edges[f, : 2 * SUBLANES] if f < 2 else activate(raw[f - 2, : 2 * SUBLANES], gain[...].reshape(1, -1))
        edges[f, : 2 * SUBLANES] = jnp.where(inside, value, jnp.zeros_like(value))
        edges[f, 2 * SUBLANES :] = jnp.zeros((SUBLANES, channels), jnp.float32)
    sums = [None] * 3
    for b in range(3):
        side = [
            jnp.concatenate([edges[f, b : b + SUBLANES], edges[f, SUBLANES + b : 2 * SUBLANES + b]], axis=0)
            .astype(jnp.bfloat16)
            for f in range(2 + count)
        ]
        for a in range(3):
            window = jnp.concatenate(side[a : a + count], axis=0)
            for c in range(3):
                part = jnp.dot(window, weight[a, b, c], preferred_element_type=jnp.float32)
                sums[c] = part if sums[c] is None else sums[c] + part
    inside = row_valid(SUBLANES, mid, top, bottom, 1)
    row = lax.broadcasted_iota(jnp.int32, (SUBLANES, 1), 0)
    blank = jnp.zeros((SUBLANES, channels), jnp.float32)
    inner, rim = [], []
    for t in range(count):
        near = [total[2 * SUBLANES * t : 2 * SUBLANES * t + SUBLANES] for total in sums]
        next_ = [total[2 * SUBLANES * t + SUBLANES : 2 * SUBLANES * (t + 1)] for total in sums]
        edge = edge_in[t] + near[1] + jnp.where(left, next_[2], next_[0])
        edge = edge + raw[t, 1 : 1 + SUBLANES] + bias[...].reshape(1, -1)
        edges[t, :SUBLANES] = jnp.where(inside, edge, blank)
        rim.append(edges.at[t])
        lines = []
        for r in range(mid):
            change = jnp.where(left, near[2][r : r + 1], near[0][r : r + 1])
            value = block_in[t, r] + jnp.where(row == jnp.where(left, BLOCK - 1, 0), change, blank)
            if r in (0, mid - 1):
                value = jnp.where(bottom if r else top, blank, value)
            lines.append(value)
        inner.append(lines)
    windows = [
        jnp.concatenate(
            [value for lines in inner for value in lines[k : k + rows]] + [line[k : k + SUBLANES] for line in rim], axis=0
        ).astype(jnp.bfloat16)
        for k in range(3)
    ]
    line, early = phase_lines(up_bias, channels)
    nothing = jnp.zeros((1, channels), jnp.float32)
    fresh = (left & (row >= BLOCK - 2)) | (jnp.logical_not(left) & (row < 2))
    size = count * rows * BLOCK
    lo, hi = SUBLANES, SUBLANES + BLOCK
    for p in range(2):
        centre, sides = phase_sums(windows, folded, p)
        for t in range(count):
            for r in range(rows):
                at = t * rows + r
                value = sides[size + t * SUBLANES + r : size + t * SUBLANES + r + 1]
                wide[p, at, lo:hi, :] = sides[at * BLOCK : (at + 1) * BLOCK]
                wide[p, at, lo - 1 : lo, :] = jnp.where(left, nothing, value)
                wide[p, at, hi : hi + 1, :] = jnp.where(left, value, nothing)
                total = centre[at * BLOCK : (at + 1) * BLOCK] + line
                total = total + jnp.where(early, wide[p, at, lo - 1 : hi - 1, :], wide[p, at, lo + 1 : hi + 1, :])
                old = jnp.where(left, done[t, 2 * r + p, cols - BLOCK :, :], done[t, 2 * r + p, :BLOCK, :])
                block[t, 2 * r + p] = jnp.where(fresh, total, old.astype(jnp.float32)).astype(jnp.bfloat16)
    for t in range(count):
        copies.append(pltpu.make_async_copy(block.at[t], out_hbm.at[t, :, strip, :], sent.at[count + t]))
        copies[-1].start()
    for copy in copies:
        copy.wait()


VMEM = pl.BlockSpec(memory_space=pltpu.VMEM)
HBM = pl.BlockSpec(memory_space=pltpu.HBM)


def call(kernel, specs, shapes, scratch, flops, *args, outs=VMEM):
    return pl.pallas_call(
        kernel,
        out_shape=shapes,
        in_specs=specs,
        out_specs=jax.tree.map(lambda _: outs, shapes),
        scratch_shapes=scratch,
        cost_estimate=pl.CostEstimate(flops=flops, transcendentals=0, bytes_accessed=0),
        compiler_params=pltpu.CompilerParams(vmem_limit_bytes=16 * 1024 * 1024),
    )(*[pltpu.with_memory_space_constraint(arg, pltpu.HBM) if spec is HBM else arg for spec, arg in zip(specs, args)])


def block(frames, cache, norm_gain, conv_weight, conv_bias, up_weight, up_bias):
    count, rows, cols, channels = frames.shape
    outputs = up_weight.shape[-1]
    cores = lax.axis_size("wa")
    f32, bf16 = jnp.float32, jnp.bfloat16
    shape = jax.ShapeDtypeStruct
    part = shape((3, HALO, cols, LANES), bf16)
    sibling = [(i, cores - 1 - i) for i in range(cores)]
    along, against, later = snake((1, -1), 0), snake((-1, 1), 0), snake((1, -1), 1)
    first, second, raw_first, raw_second, act = call(
        pack_kernel, [HBM] * 3, (part, part, part, part, shape(frames.shape, bf16)),
        (pltpu.VMEM(frames.shape, bf16), pltpu.VMEM(cache.shape, bf16), pltpu.VMEM(norm_gain.shape, f32),
         pltpu.SemaphoreType.DMA((3,))),
        COST, frames, cache, norm_gain,
    )
    main_a = lax.ppermute(first, "ta", ring("ta"))
    main_b = lax.ppermute(second, "ta", ring("ta"))
    prev_a = lax.ppermute(second, AXES, later)
    own_a = lax.ppermute(raw_first, AXES, along)
    own_b = lax.ppermute(raw_second, AXES, against)
    prev_b = lax.ppermute(main_a, AXES, against)
    sib = call(
        near_kernel, [VMEM] * 8, shape((3, 4 * rows, BLOCK, LANES), bf16), (), 0,
        main_a, main_b, prev_a, prev_b, own_a, own_b, raw_first, raw_second,
    )
    sib = lax.ppermute(sib, "wa", sibling)
    mid, all_rows = rows + 2, rows + 2 * HALO
    body_shape = shape((count, mid, cols, channels), f32)
    edge_shape = shape((count, SUBLANES, channels), f32)
    shift = pltpu.VMEM((mid, cols + 2 * SUBLANES, channels), f32)
    tile = pltpu.VMEM((2, rows, cols, channels), bf16)
    halo = pltpu.VMEM((2, 2 * HALO, cols, channels), bf16)
    body, edge = call(
        first_kernel, [VMEM] * 5, (body_shape, edge_shape), (tile, shift, shift),
        10**9, raw_first, raw_second, act, conv_weight, conv_bias,
    )
    body, edge = call(
        second_kernel, [VMEM] * 8, (body_shape, edge_shape), (tile, halo, halo, shift, shift),
        10**9, main_a, main_b, own_a, own_b, conv_weight, norm_gain, body, edge,
    )
    folded = call(fold_kernel, [VMEM], shape((8, channels, 2 * outputs), bf16), (), 10**8, up_weight)
    out_shape = (count, 2 * rows, cols, 2 * outputs)
    block, edge, out = call(
        third_kernel, [VMEM] * 7,
        (shape((count, mid, BLOCK, channels), f32), edge_shape, shape(out_shape, bf16)),
        (halo, shift, shift, pltpu.VMEM((count, mid, cols, channels), bf16),
         pltpu.VMEM((2, rows, cols + 2 * SUBLANES, channels), f32)), 10**9,
        prev_a, prev_b, conv_weight, folded, up_bias, body, edge,
    )
    near = pltpu.VMEM((2, all_rows, BLOCK, channels), bf16)
    return call(
        last_kernel, [VMEM] * 9, shape(out_shape, bf16),
        (near, near, pltpu.VMEM((2 + count, 3 * SUBLANES, channels), f32), pltpu.VMEM((count, 3 * SUBLANES, channels), f32),
         pltpu.VMEM((2, count * rows, BLOCK + 2 * SUBLANES, channels), f32),
         pltpu.VMEM((count, 2 * rows, BLOCK, 2 * outputs), bf16), pltpu.SemaphoreType.DMA((2 * count,))),
        10**9, sib, conv_weight, block, edge, folded, norm_gain, conv_bias, up_bias, out, outs=HBM,
    )


def solution(mesh):
    return jax.shard_map(
        block,
        mesh=mesh,
        in_specs=(
            P(("clips", "ta"), "ha", "wa", None),
            P("clips", "ha", "wa", None),
            P(),
            P(),
            P(),
            P(),
            P(),
        ),
        out_specs=P(("clips", "ta"), "ha", "wa", None),
        check_vma=False,
    )
```

```python
import functools

import jax
import jax.numpy as jnp
from jax import lax
from jax.experimental import pallas as pl
from jax.experimental.pallas import tpu as pltpu
from jax.sharding import PartitionSpec as P


EPS = 1e-06
HALO = 2
LANES = 128
COST = 8 * 10**8
BLOCK = 8
SUBLANES = 8
AXES = ("ha", "ta", "wa")


def ring(axis):
    count = lax.axis_size(axis)
    return [(i, (i + 1) % count) for i in range(count)]


def snake(towards, later):
    chips, steps, cores = (lax.axis_size(axis) for axis in AXES)
    pairs = []
    for h in range(chips):
        for t in range(steps):
            for w in range(cores):
                step, target, core = (t + later) % steps, h + towards[w], w
                if not 0 <= target < chips:
                    target, core = h, cores - 1 - w
                pairs.append(((h * steps + t) * cores + w, (target * steps + step) * cores + core))
    return pairs


def activate(values, gain):
    wide = values.astype(jnp.float32)
    scale = lax.rsqrt(jnp.sum(wide * wide, axis=-1, keepdims=True) / wide.shape[-1] + EPS)
    v = wide * scale * gain
    return v / (1.0 + jnp.exp(-v))


def packed(cells):
    rest = jnp.concatenate([cells[0, :, :, LANES:], cells[1, :, :, LANES:]], axis=-1)
    return jnp.stack([cells[0, :, :, :LANES], cells[1, :, :, :LANES], rest])


def fetch(sources, targets, arrived):
    copies = [pltpu.make_async_copy(*pair, arrived.at[i]) for i, pair in enumerate(zip(sources, targets))]
    for copy in copies:
        copy.start()
    return copies


def pack_kernel(frames_hbm, cache_hbm, gain_hbm, first, second, raw_first, raw_second, act,
                frames, cache, gain, arrived):
    left = lax.axis_index("wa") == 0
    last = lax.axis_index("ta") == lax.axis_size("ta") - 1
    rows = frames.shape[1]
    pieces = [(f, r) for f in range(frames.shape[0]) for r in range(rows)]
    sources = [gain_hbm] + [frames_hbm.at[f, r] for f, r in pieces] + [cache_hbm.at[f, r] for f, r in pieces]
    targets = [gain] + [frames.at[f, r] for f, r in pieces] + [cache.at[f, r] for f, r in pieces]
    copies = fetch(sources, targets, arrived)
    for copy in copies[: 1 + len(pieces)]:
        copy.wait()
    cells = frames[...]
    active = activate(cells, gain[...].reshape(1, -1)).astype(jnp.bfloat16)
    act[...] = active
    for copy in copies[1 + len(pieces) :]:
        copy.wait()
    sent = packed(jnp.where(last, cache[...], active))
    first[...] = jnp.where(left, sent[:, :HALO], sent[:, HALO:])
    second[...] = jnp.where(left, sent[:, HALO:], sent[:, :HALO])
    sent = packed(cells)
    raw_first[...] = jnp.where(left, sent[:, HALO:], sent[:, :HALO])
    raw_second[...] = jnp.where(left, sent[:, :HALO], sent[:, HALO:])


def place():
    chip = lax.axis_index("ha")
    core = lax.axis_index("wa")
    return core == 0, core, chip == 0, chip == lax.axis_size("ha") - 1


def unpack(planes, cells, start):
    rows = planes.shape[1]
    rest = cells.shape[-1] - LANES
    for f in range(2):
        cells[f, pl.ds(start, rows), :, :LANES] = planes[f, :, :, :]
        cells[f, pl.ds(start, rows), :, LANES:] = planes[2, :, :, f * rest : (f + 1) * rest]


def clear_outside(cells, top, bottom):
    zero = jnp.zeros((2, HALO) + cells.shape[2:], cells.dtype)
    cells[:, :HALO] = jnp.where(top, zero, cells[:, :HALO])
    cells[:, HALO:] = jnp.where(bottom, zero, cells[:, HALO:])


def row_sums(inner, outer, weight, c, mid):
    parts = [[] for _ in range(mid)]
    for b in range(3):
        if inner:
            rows, cols, channels = inner[0][1].shape
            total = None
            for a, cells in inner:
                part = jnp.dot(cells.reshape(rows * cols, channels), weight[a, b, c], preferred_element_type=jnp.float32)
                total = part if total is None else total + part
            for r in range(rows):
                parts[r + HALO - b].append(total[r * cols : (r + 1) * cols])
        if outer:
            cols, channels = outer[0][1].shape[1:]
            total = None
            for a, cells in outer:
                window = cells[b : b + HALO].reshape(HALO * cols, channels)
                part = jnp.dot(window, weight[a, b, c], preferred_element_type=jnp.float32)
                total = part if total is None else total + part
            for r, target in enumerate(((0, 1), (0, mid - 1), (mid - 2, mid - 1))[b]):
                parts[target].append(total[r * cols : (r + 1) * cols])
    return [functools.reduce(jnp.add, part) if part else None for part in parts]


def add_taps(inner, outer, weight, base, rim, before, after, left):
    mid = len(base)
    channels = weight.shape[-1]
    lo, hi = SUBLANES, before.shape[1] - SUBLANES
    zero = jnp.zeros((1, channels), jnp.float32)
    first, second, third = [row_sums(inner, outer, weight, c, mid) for c in range(3)]
    total, line = [], []
    for r in range(mid):
        if second[r] is None:
            total.append(base[r])
            line.append(zero)
            continue
        before[r, lo - 1 : lo, :] = zero
        after[r, hi : hi + 1, :] = zero
        before[r, lo:hi, :] = first[r]
        after[r, lo:hi, :] = third[r]
        value = second[r] + before[r, lo - 1 : hi - 1, :] + after[r, lo + 1 : hi + 1, :]
        total.append(value if base[r] is None else base[r] + value)
        line.append(jnp.where(left, before[r, hi - 1 : hi, :], after[r, lo : lo + 1, :]))
    line = jnp.concatenate(line + [zero] * (SUBLANES - mid), axis=0)
    return total, line if rim is None else rim + line


def first_kernel(raw_first, raw_second, act, weight, bias, body_out, edge_out, frames, before, after):
    left, core, _, _ = place()
    count, mid, cols, channels = body_out.shape
    unpack(raw_first, frames, (1 - core) * HALO)
    unpack(raw_second, frames, core * HALO)
    line = bias[...].reshape(1, -1)
    none = jnp.broadcast_to(line, (cols, channels))
    for t in range(count):
        inner = [(a, act[t + a - 2]) for a in range(3) if 0 <= t + a - 2]
        base = [none] + [frames[t, r].astype(jnp.float32) + line for r in range(mid - 2)] + [none]
        total, edge = add_taps(inner, [], weight, base, None, before, after, left)
        for r in range(mid):
            body_out[t, r] = total[r]
        edge_out[t] = edge


def second_kernel(main_a, main_b, own_a, own_b, weight, gain, body_in, edge_in, body_out, edge_out,
                  main, raw, halo, before, after):
    left, core, top, bottom = place()
    count, mid, _, _ = body_in.shape
    unpack(main_a, main, core * HALO)
    unpack(main_b, main, (1 - core) * HALO)
    unpack(own_a, raw, core * HALO)
    unpack(own_b, raw, (1 - core) * HALO)
    halo[...] = activate(raw[...], gain[...].reshape(1, -1)).astype(jnp.bfloat16)
    clear_outside(halo, top, bottom)
    for t in range(count):
        inner = [(a, main[t + a]) for a in range(3) if t + a < 2]
        outer = [(a, halo.at[t + a - 2]) for a in range(3) if 0 <= t + a - 2]
        base = [body_in[t, r] for r in range(mid)]
        base[0] = base[0] + raw[t, HALO - 1].astype(jnp.float32)
        base[-1] = base[-1] + raw[t, HALO].astype(jnp.float32)
        total, edge = add_taps(inner, outer, weight, base, edge_in[t], before, after, left)
        for r in range(mid):
            body_out[t, r] = total[r]
        edge_out[t] = edge


def fold_kernel(weight, folded):
    taps = [[weight[a, b].astype(jnp.float32) for b in range(3)] for a in range(3)]
    columns = []
    for rows in ((0,), (1, 2), (0, 1), (2,)):
        columns.append([functools.reduce(jnp.add, [taps[a][b] for a in rows]) for b in range(3)])
    for i, (one, two, three) in enumerate(columns):
        folded[2 * i] = jnp.concatenate([two + three, one + two], axis=-1).astype(jnp.bfloat16)
        folded[2 * i + 1] = jnp.concatenate([one, three], axis=-1).astype(jnp.bfloat16)


def phase_sums(windows, folded, p):
    centre = sides = None
    for k in range(2):
        i = 2 * (2 * p + k)
        one = jnp.dot(windows[p + k], folded[i], preferred_element_type=jnp.float32)
        two = jnp.dot(windows[p + k], folded[i + 1], preferred_element_type=jnp.float32)
        centre = one if centre is None else centre + one
        sides = two if sides is None else sides + two
    return centre, sides


def phase_lines(bias, channels):
    line = bias[...].reshape(1, -1)
    early = lax.broadcasted_iota(jnp.int32, (1, channels), 1) < channels // 2
    return jnp.concatenate([line, line], axis=-1), early


def third_kernel(prev_a, prev_b, weight, folded, up_bias, body_in, edge_in, block_out, edge_out, out,
                 halo, before, after, res, wide):
    left, core, top, bottom = place()
    count, mid, cols, channels = body_in.shape
    unpack(prev_a, halo, core * HALO)
    unpack(prev_b, halo, (1 - core) * HALO)
    clear_outside(halo, top, bottom)
    for t in range(count):
        outer = [(a, halo.at[t + a]) for a in range(3) if t + a < 2]
        base = [body_in[t, r] for r in range(mid)]
        total, line = add_taps([], outer, weight, base, edge_in[t], before, after, left)
        edge_out[t] = line
        for r in range(mid):
            block_out[t, r] = jnp.where(left, total[r][cols - BLOCK :], total[r][:BLOCK])
            value = total[r].astype(jnp.bfloat16)
            if r in (0, mid - 1):
                value = jnp.where(bottom if r else top, jnp.zeros_like(value), value)
            res[t, r] = value
    rows = mid - 2
    lo, hi = SUBLANES, SUBLANES + cols
    line, early = phase_lines(up_bias, channels)
    nothing = jnp.zeros((1, channels), jnp.float32)
    for t in range(count):
        windows = [res[t, k : k + rows].reshape(rows * cols, channels) for k in range(3)]
        for p in range(2):
            centre, sides = phase_sums(windows, folded, p)
            for r in range(rows):
                wide[p, r, lo:hi, :] = sides[r * cols : (r + 1) * cols]
                wide[p, r, lo - 1 : lo, :] = nothing
                wide[p, r, hi : hi + 1, :] = nothing
                total = centre[r * cols : (r + 1) * cols]
                total = total + jnp.where(early, wide[p, r, lo - 1 : hi - 1, :], wide[p, r, lo + 1 : hi + 1, :])
                out[t, 2 * r + p] = (total + line).astype(jnp.bfloat16)


def edge_columns(near, edges, left):
    frames, rows = near.shape[0], near.shape[1]
    for f in range(frames):
        for r in range(rows):
            block = near[f, r].astype(jnp.float32)
            for s in range(HALO):
                line = jnp.where(left, block[s : s + 1], block[BLOCK - 1 - s : BLOCK - s])
                edges[f, s * rows + r : s * rows + r + 1, :] = line
        edges[f, HALO * rows :, :] = jnp.zeros((SUBLANES, near.shape[-1]), jnp.float32)


def near_kernel(*refs):
    left = lax.axis_index("wa") == 0
    out, start = refs[-1], 0
    for part in refs[:-1]:
        rows, cols = part.shape[1:3]
        out[:, start : start + rows] = jnp.where(left, part[:, :, cols - BLOCK :, :], part[:, :, :BLOCK, :])
        start += rows


def row_valid(count, rows, top, bottom, halo):
    row = lax.broadcasted_iota(jnp.int32, (count, 1), 0) % SUBLANES
    return jnp.logical_not((top & (row < halo)) | (bottom & (row >= rows - halo)))


def last_kernel(sib, weight, block_in, edge_in, folded, gain, bias, up_bias, done, out_hbm,
                near_prev, near_own, edges, raw, wide, block, sent):
    left, core, top, bottom = place()
    count, mid, _, channels = block_in.shape
    rows = mid - 2
    cols = done.shape[2]
    far = rows + HALO
    rest = pl.ds(pl.multiple_of(core * BLOCK, BLOCK), cols - BLOCK)
    strip = pl.ds(pl.multiple_of((1 - core) * (cols - BLOCK), BLOCK), BLOCK)
    copies = [
        pltpu.make_async_copy(done.at[t, :, rest, :], out_hbm.at[t, :, rest, :], sent.at[t]) for t in range(count)
    ]
    for copy in copies:
        copy.start()
    starts = (HALO + (1 - core) * HALO, HALO + core * HALO, (1 - core) * far, core * far)
    for i, start in enumerate(starts):
        unpack(sib[:, i * HALO : (i + 1) * HALO], near_prev, start)
    starts = ((1 - core) * far, core * far, HALO + core * HALO, HALO + (1 - core) * HALO)
    for i, start in enumerate(starts):
        unpack(sib[:, 4 * HALO + i * HALO : 4 * HALO + (i + 1) * HALO], near_own, start)
    edge_columns(near_prev, edges.at[:2], left)
    edge_columns(near_own, raw, left)
    inside = row_valid(2 * SUBLANES, SUBLANES, top, bottom, HALO)
    for f in range(2 + count):
        value = edges[f, : 2 * SUBLANES] if f < 2 else activate(raw[f - 2, : 2 * SUBLANES], gain[...].reshape(1, -1))
        edges[f, : 2 * SUBLANES] = jnp.where(inside, value, jnp.zeros_like(value))
        edges[f, 2 * SUBLANES :] = jnp.zeros((SUBLANES, channels), jnp.float32)
    sums = [None] * 3
    for b in range(3):
        side = [
            jnp.concatenate([edges[f, b : b + SUBLANES], edges[f, SUBLANES + b : 2 * SUBLANES + b]], axis=0)
            .astype(jnp.bfloat16)
            for f in range(2 + count)
        ]
        for a in range(3):
            window = jnp.concatenate(side[a : a + count], axis=0)
            for c in range(3):
                part = jnp.dot(window, weight[a, b, c], preferred_element_type=jnp.float32)
                sums[c] = part if sums[c] is None else sums[c] + part
    inside = row_valid(SUBLANES, mid, top, bottom, 1)
    row = lax.broadcasted_iota(jnp.int32, (SUBLANES, 1), 0)
    blank = jnp.zeros((SUBLANES, channels), jnp.float32)
    inner, rim = [], []
    for t in range(count):
        near = [total[2 * SUBLANES * t : 2 * SUBLANES * t + SUBLANES] for total in sums]
        next_ = [total[2 * SUBLANES * t + SUBLANES : 2 * SUBLANES * (t + 1)] for total in sums]
        edge = edge_in[t] + near[1] + jnp.where(left, next_[2], next_[0])
        edge = edge + raw[t, 1 : 1 + SUBLANES] + bias[...].reshape(1, -1)
        edges[t, :SUBLANES] = jnp.where(inside, edge, blank)
        rim.append(edges.at[t])
        lines = []
        for r in range(mid):
            change = jnp.where(left, near[2][r : r + 1], near[0][r : r + 1])
            value = block_in[t, r] + jnp.where(row == jnp.where(left, BLOCK - 1, 0), change, blank)
            if r in (0, mid - 1):
                value = jnp.where(bottom if r else top, blank, value)
            lines.append(value)
        inner.append(lines)
    windows = [
        jnp.concatenate(
            [value for lines in inner for value in lines[k : k + rows]] + [line[k : k + SUBLANES] for line in rim], axis=0
        ).astype(jnp.bfloat16)
        for k in range(3)
    ]
    line, early = phase_lines(up_bias, channels)
    nothing = jnp.zeros((1, channels), jnp.float32)
    fresh = (left & (row >= BLOCK - 2)) | (jnp.logical_not(left) & (row < 2))
    size = count * rows * BLOCK
    lo, hi = SUBLANES, SUBLANES + BLOCK
    for p in range(2):
        centre, sides = phase_sums(windows, folded, p)
        for t in range(count):
            for r in range(rows):
                at = t * rows + r
                value = sides[size + t * SUBLANES + r : size + t * SUBLANES + r + 1]
                wide[p, at, lo:hi, :] = sides[at * BLOCK : (at + 1) * BLOCK]
                wide[p, at, lo - 1 : lo, :] = jnp.where(left, nothing, value)
                wide[p, at, hi : hi + 1, :] = jnp.where(left, value, nothing)
                total = centre[at * BLOCK : (at + 1) * BLOCK] + line
                total = total + jnp.where(early, wide[p, at, lo - 1 : hi - 1, :], wide[p, at, lo + 1 : hi + 1, :])
                old = jnp.where(left, done[t, 2 * r + p, cols - BLOCK :, :], done[t, 2 * r + p, :BLOCK, :])
                block[t, 2 * r + p] = jnp.where(fresh, total, old.astype(jnp.float32)).astype(jnp.bfloat16)
    for t in range(count):
        copies.append(pltpu.make_async_copy(block.at[t], out_hbm.at[t, :, strip, :], sent.at[count + t]))
        copies[-1].start()
    for copy in copies:
        copy.wait()


VMEM = pl.BlockSpec(memory_space=pltpu.VMEM)
HBM = pl.BlockSpec(memory_space=pltpu.HBM)


def call(kernel, specs, shapes, scratch, flops, *args, outs=VMEM):
    return pl.pallas_call(
        kernel,
        out_shape=shapes,
        in_specs=specs,
        out_specs=jax.tree.map(lambda _: outs, shapes),
        scratch_shapes=scratch,
        cost_estimate=pl.CostEstimate(flops=flops, transcendentals=0, bytes_accessed=0),
        compiler_params=pltpu.CompilerParams(vmem_limit_bytes=16 * 1024 * 1024),
    )(*[pltpu.with_memory_space_constraint(arg, pltpu.HBM) if spec is HBM else arg for spec, arg in zip(specs, args)])


def block(frames, cache, norm_gain, conv_weight, conv_bias, up_weight, up_bias):
    count, rows, cols, channels = frames.shape
    outputs = up_weight.shape[-1]
    cores = lax.axis_size("wa")
    f32, bf16 = jnp.float32, jnp.bfloat16
    shape = jax.ShapeDtypeStruct
    part = shape((3, HALO, cols, LANES), bf16)
    sibling = [(i, cores - 1 - i) for i in range(cores)]
    along, against, later = snake((1, -1), 0), snake((-1, 1), 0), snake((1, -1), 1)
    first, second, raw_first, raw_second, act = call(
        pack_kernel, [HBM] * 3, (part, part, part, part, shape(frames.shape, bf16)),
        (pltpu.VMEM(frames.shape, bf16), pltpu.VMEM(cache.shape, bf16), pltpu.VMEM(norm_gain.shape, f32),
         pltpu.SemaphoreType.DMA((1 + 2 * count * rows,))),
        COST, frames, cache, norm_gain,
    )
    main_a = lax.ppermute(first, "ta", ring("ta"))
    main_b = lax.ppermute(second, "ta", ring("ta"))
    prev_a = lax.ppermute(second, AXES, later)
    own_a = lax.ppermute(raw_first, AXES, along)
    own_b = lax.ppermute(raw_second, AXES, against)
    prev_b = lax.ppermute(main_a, AXES, against)
    sib = call(
        near_kernel, [VMEM] * 8, shape((3, 4 * rows, BLOCK, LANES), bf16), (), 0,
        main_a, main_b, prev_a, prev_b, own_a, own_b, raw_first, raw_second,
    )
    sib = lax.ppermute(sib, "wa", sibling)
    mid, all_rows = rows + 2, rows + 2 * HALO
    body_shape = shape((count, mid, cols, channels), f32)
    edge_shape = shape((count, SUBLANES, channels), f32)
    shift = pltpu.VMEM((mid, cols + 2 * SUBLANES, channels), f32)
    tile = pltpu.VMEM((2, rows, cols, channels), bf16)
    halo = pltpu.VMEM((2, 2 * HALO, cols, channels), bf16)
    body, edge = call(
        first_kernel, [VMEM] * 5, (body_shape, edge_shape), (tile, shift, shift),
        10**9, raw_first, raw_second, act, conv_weight, conv_bias,
    )
    body, edge = call(
        second_kernel, [VMEM] * 8, (body_shape, edge_shape), (tile, halo, halo, shift, shift),
        10**9, main_a, main_b, own_a, own_b, conv_weight, norm_gain, body, edge,
    )
    folded = call(fold_kernel, [VMEM], shape((8, channels, 2 * outputs), bf16), (), 3 * 10**9, up_weight)
    out_shape = (count, 2 * rows, cols, 2 * outputs)
    block, edge, out = call(
        third_kernel, [VMEM] * 7,
        (shape((count, mid, BLOCK, channels), f32), edge_shape, shape(out_shape, bf16)),
        (halo, shift, shift, pltpu.VMEM((count, mid, cols, channels), bf16),
         pltpu.VMEM((2, rows, cols + 2 * SUBLANES, channels), f32)), 10**9,
        prev_a, prev_b, conv_weight, folded, up_bias, body, edge,
    )
    near = pltpu.VMEM((2, all_rows, BLOCK, channels), bf16)
    return call(
        last_kernel, [VMEM] * 9, shape(out_shape, bf16),
        (near, near, pltpu.VMEM((2 + count, 3 * SUBLANES, channels), f32), pltpu.VMEM((count, 3 * SUBLANES, channels), f32),
         pltpu.VMEM((2, count * rows, BLOCK + 2 * SUBLANES, channels), f32),
         pltpu.VMEM((count, 2 * rows, BLOCK, 2 * outputs), bf16), pltpu.SemaphoreType.DMA((2 * count,))),
        10**9, sib, conv_weight, block, edge, folded, norm_gain, conv_bias, up_bias, out, outs=HBM,
    )


def solution(mesh):
    return jax.shard_map(
        block,
        mesh=mesh,
        in_specs=(
            P(("clips", "ta"), "ha", "wa", None),
            P("clips", "ha", "wa", None),
            P(),
            P(),
            P(),
            P(),
            P(),
        ),
        out_specs=P(("clips", "ta"), "ha", "wa", None),
        check_vma=False,
    )
```

```python
import functools

import jax
import jax.numpy as jnp
from jax import lax
from jax.experimental import pallas as pl
from jax.experimental.pallas import tpu as pltpu
from jax.sharding import PartitionSpec as P


EPS = 1e-06
HALO = 2
LANES = 128
COST = 8 * 10**8
BLOCK = 8
SUBLANES = 8
AXES = ("ha", "ta", "wa")


def ring(axis):
    count = lax.axis_size(axis)
    return [(i, (i + 1) % count) for i in range(count)]


def snake(towards, later):
    chips, steps, cores = (lax.axis_size(axis) for axis in AXES)
    pairs = []
    for h in range(chips):
        for t in range(steps):
            for w in range(cores):
                step, target, core = (t + later) % steps, h + towards[w], w
                if not 0 <= target < chips:
                    target, core = h, cores - 1 - w
                pairs.append(((h * steps + t) * cores + w, (target * steps + step) * cores + core))
    return pairs


def activate(values, gain):
    wide = values.astype(jnp.float32)
    scale = lax.rsqrt(jnp.sum(wide * wide, axis=-1, keepdims=True) / wide.shape[-1] + EPS)
    v = wide * scale * gain
    return v / (1.0 + jnp.exp(-v))


def packed(cells):
    rest = jnp.concatenate([cells[0, :, :, LANES:], cells[1, :, :, LANES:]], axis=-1)
    return jnp.stack([cells[0, :, :, :LANES], cells[1, :, :, :LANES], rest])


def fetch(sources, targets, arrived):
    copies = [pltpu.make_async_copy(*pair, arrived.at[i]) for i, pair in enumerate(zip(sources, targets))]
    for copy in copies:
        copy.start()
    return copies


def pack_kernel(frames_hbm, cache_hbm, gain_hbm, first, second, raw_first, raw_second, act,
                frames, cache, gain, arrived):
    left = lax.axis_index("wa") == 0
    last = lax.axis_index("ta") == lax.axis_size("ta") - 1
    rows = frames.shape[1]
    pieces = [(f, r) for f in range(frames.shape[0]) for r in range(rows)]
    sources = [gain_hbm] + [frames_hbm.at[f, r] for f, r in pieces] + [cache_hbm.at[f, r] for f, r in pieces]
    targets = [gain] + [frames.at[f, r] for f, r in pieces] + [cache.at[f, r] for f, r in pieces]
    copies = fetch(sources, targets, arrived)
    for copy in copies[: 1 + len(pieces)]:
        copy.wait()
    cells = frames[...]
    active = activate(cells, gain[...].reshape(1, -1)).astype(jnp.bfloat16)
    act[...] = active
    for copy in copies[1 + len(pieces) :]:
        copy.wait()
    sent = packed(jnp.where(last, cache[...], active))
    first[...] = jnp.where(left, sent[:, :HALO], sent[:, HALO:])
    second[...] = jnp.where(left, sent[:, HALO:], sent[:, :HALO])
    sent = packed(cells)
    raw_first[...] = jnp.where(left, sent[:, HALO:], sent[:, :HALO])
    raw_second[...] = jnp.where(left, sent[:, :HALO], sent[:, HALO:])


def place():
    chip = lax.axis_index("ha")
    core = lax.axis_index("wa")
    return core == 0, core, chip == 0, chip == lax.axis_size("ha") - 1


def unpack(planes, cells, start):
    rows = planes.shape[1]
    rest = cells.shape[-1] - LANES
    for f in range(2):
        cells[f, pl.ds(start, rows), :, :LANES] = planes[f, :, :, :]
        cells[f, pl.ds(start, rows), :, LANES:] = planes[2, :, :, f * rest : (f + 1) * rest]


def clear_outside(cells, top, bottom):
    zero = jnp.zeros((2, HALO) + cells.shape[2:], cells.dtype)
    cells[:, :HALO] = jnp.where(top, zero, cells[:, :HALO])
    cells[:, HALO:] = jnp.where(bottom, zero, cells[:, HALO:])


def row_sums(inner, outer, weight, c, mid):
    parts = [[] for _ in range(mid)]
    for b in range(3):
        if inner:
            rows, cols, channels = inner[0][1].shape
            total = None
            for a, cells in inner:
                part = jnp.dot(cells.reshape(rows * cols, channels), weight[a, b, c], preferred_element_type=jnp.float32)
                total = part if total is None else total + part
            for r in range(rows):
                parts[r + HALO - b].append(total[r * cols : (r + 1) * cols])
        if outer:
            cols, channels = outer[0][1].shape[1:]
            total = None
            for a, cells in outer:
                window = cells[b : b + HALO].reshape(HALO * cols, channels)
                part = jnp.dot(window, weight[a, b, c], preferred_element_type=jnp.float32)
                total = part if total is None else total + part
            for r, target in enumerate(((0, 1), (0, mid - 1), (mid - 2, mid - 1))[b]):
                parts[target].append(total[r * cols : (r + 1) * cols])
    return [functools.reduce(jnp.add, part) if part else None for part in parts]


def add_taps(inner, outer, weight, base, rim, before, after, left):
    mid = len(base)
    channels = weight.shape[-1]
    lo, hi = SUBLANES, before.shape[1] - SUBLANES
    zero = jnp.zeros((1, channels), jnp.float32)
    first, second, third = [row_sums(inner, outer, weight, c, mid) for c in range(3)]
    total, line = [], []
    for r in range(mid):
        if second[r] is None:
            total.append(base[r])
            line.append(zero)
            continue
        before[r, lo - 1 : lo, :] = zero
        after[r, hi : hi + 1, :] = zero
        before[r, lo:hi, :] = first[r]
        after[r, lo:hi, :] = third[r]
        value = second[r] + before[r, lo - 1 : hi - 1, :] + after[r, lo + 1 : hi + 1, :]
        total.append(value if base[r] is None else base[r] + value)
        line.append(jnp.where(left, before[r, hi - 1 : hi, :], after[r, lo : lo + 1, :]))
    line = jnp.concatenate(line + [zero] * (SUBLANES - mid), axis=0)
    return total, line if rim is None else rim + line


def first_kernel(raw_first, raw_second, act, weight, bias, body_out, edge_out, frames, before, after):
    left, core, _, _ = place()
    count, mid, cols, channels = body_out.shape
    unpack(raw_first, frames, (1 - core) * HALO)
    unpack(raw_second, frames, core * HALO)
    line = bias[...].reshape(1, -1)
    none = jnp.broadcast_to(line, (cols, channels))
    for t in range(count):
        inner = [(a, act[t + a - 2]) for a in range(3) if 0 <= t + a - 2]
        base = [none] + [frames[t, r].astype(jnp.float32) + line for r in range(mid - 2)] + [none]
        total, edge = add_taps(inner, [], weight, base, None, before, after, left)
        for r in range(mid):
            body_out[t, r] = total[r]
        edge_out[t] = edge


def second_kernel(main_a, main_b, own_a, own_b, weight, gain, body_in, edge_in, body_out, edge_out,
                  main, raw, halo, before, after):
    left, core, top, bottom = place()
    count, mid, _, _ = body_in.shape
    unpack(main_a, main, core * HALO)
    unpack(main_b, main, (1 - core) * HALO)
    unpack(own_a, raw, core * HALO)
    unpack(own_b, raw, (1 - core) * HALO)
    halo[...] = activate(raw[...], gain[...].reshape(1, -1)).astype(jnp.bfloat16)
    clear_outside(halo, top, bottom)
    for t in range(count):
        inner = [(a, main[t + a]) for a in range(3) if t + a < 2]
        outer = [(a, halo.at[t + a - 2]) for a in range(3) if 0 <= t + a - 2]
        base = [body_in[t, r] for r in range(mid)]
        base[0] = base[0] + raw[t, HALO - 1].astype(jnp.float32)
        base[-1] = base[-1] + raw[t, HALO].astype(jnp.float32)
        total, edge = add_taps(inner, outer, weight, base, edge_in[t], before, after, left)
        for r in range(mid):
            body_out[t, r] = total[r]
        edge_out[t] = edge


def fold_kernel(weight, folded):
    taps = [[weight[a, b].astype(jnp.float32) for b in range(3)] for a in range(3)]
    columns = []
    for rows in ((0,), (1, 2), (0, 1), (2,)):
        columns.append([functools.reduce(jnp.add, [taps[a][b] for a in rows]) for b in range(3)])
    for i, (one, two, three) in enumerate(columns):
        folded[2 * i] = jnp.concatenate([two + three, one + two], axis=-1).astype(jnp.bfloat16)
        folded[2 * i + 1] = jnp.concatenate([one, three], axis=-1).astype(jnp.bfloat16)


def phase_sums(windows, folded, p):
    centre = sides = None
    for k in range(2):
        i = 2 * (2 * p + k)
        one = jnp.dot(windows[p + k], folded[i], preferred_element_type=jnp.float32)
        two = jnp.dot(windows[p + k], folded[i + 1], preferred_element_type=jnp.float32)
        centre = one if centre is None else centre + one
        sides = two if sides is None else sides + two
    return centre, sides


def phase_lines(bias, channels):
    line = bias[...].reshape(1, -1)
    early = lax.broadcasted_iota(jnp.int32, (1, channels), 1) < channels // 2
    return jnp.concatenate([line, line], axis=-1), early


def third_kernel(prev_a, prev_b, weight, folded, up_bias, body_in, edge_in, block_out, edge_out, out,
                 halo, before, after, res, wide):
    left, core, top, bottom = place()
    count, mid, cols, channels = body_in.shape
    unpack(prev_a, halo, core * HALO)
    unpack(prev_b, halo, (1 - core) * HALO)
    clear_outside(halo, top, bottom)
    for t in range(count):
        outer = [(a, halo.at[t + a]) for a in range(3) if t + a < 2]
        base = [body_in[t, r] for r in range(mid)]
        total, line = add_taps([], outer, weight, base, edge_in[t], before, after, left)
        edge_out[t] = line
        for r in range(mid):
            block_out[t, r] = jnp.where(left, total[r][cols - BLOCK :], total[r][:BLOCK])
            value = total[r].astype(jnp.bfloat16)
            if r in (0, mid - 1):
                value = jnp.where(bottom if r else top, jnp.zeros_like(value), value)
            res[t, r] = value
    rows = mid - 2
    lo, hi = SUBLANES, SUBLANES + cols
    line, early = phase_lines(up_bias, channels)
    nothing = jnp.zeros((1, channels), jnp.float32)
    for t in range(count):
        windows = [res[t, k : k + rows].reshape(rows * cols, channels) for k in range(3)]
        for p in range(2):
            centre, sides = phase_sums(windows, folded, p)
            for r in range(rows):
                wide[p, r, lo:hi, :] = sides[r * cols : (r + 1) * cols]
                wide[p, r, lo - 1 : lo, :] = nothing
                wide[p, r, hi : hi + 1, :] = nothing
                total = centre[r * cols : (r + 1) * cols]
                total = total + jnp.where(early, wide[p, r, lo - 1 : hi - 1, :], wide[p, r, lo + 1 : hi + 1, :])
                out[t, 2 * r + p] = (total + line).astype(jnp.bfloat16)


def edge_columns(near, rows, edges, left):
    for f in range(near.shape[0]):
        for i, r in enumerate(rows):
            block = near[f, i].astype(jnp.float32)
            for s in range(HALO):
                line = jnp.where(left, block[s : s + 1], block[BLOCK - 1 - s : BLOCK - s])
                edges[f, s * SUBLANES + r : s * SUBLANES + r + 1, :] = line


def edge_sides(edges, f):
    return [
        jnp.concatenate([edges[f, b : b + SUBLANES], edges[f, SUBLANES + b : 2 * SUBLANES + b]], axis=0)
        .astype(jnp.bfloat16)
        for b in range(3)
    ]


def edge_sums(sides, a, weight):
    sums = [None] * 3
    for b in range(3):
        window = jnp.concatenate([side[b] for side in sides], axis=0)
        for c in range(3):
            part = jnp.dot(window, weight[a, b, c], preferred_element_type=jnp.float32)
            sums[c] = part if sums[c] is None else sums[c] + part
    return sums


def edge_kernel(sib, weight, gain, bias, sums_out, raw_out, near_prev, near_own, edges, raw):
    left, core, top, bottom = place()
    count = raw_out.shape[0]
    rows = near_prev.shape[1]
    far = rows + HALO
    starts = (near_prev, (1 - core) * HALO), (near_prev, core * HALO), (near_own, (1 - core) * far), (near_own, core * far)
    starts += (near_own, HALO + core * HALO), (near_own, HALO + (1 - core) * HALO)
    for i, (cells, start) in enumerate(starts):
        unpack(sib[:, i * HALO : (i + 1) * HALO], cells, start)
    edges[...] = jnp.zeros(edges.shape, jnp.float32)
    raw[...] = jnp.zeros(raw.shape, jnp.float32)
    edge_columns(near_prev, range(HALO, far), edges.at[:2], left)
    edge_columns(near_own, range(rows + 2 * HALO), raw, left)
    inside = row_valid(2 * SUBLANES, SUBLANES, top, bottom, HALO)
    for f in range(count):
        value = activate(raw[f, : 2 * SUBLANES], gain[...].reshape(1, -1))
        edges[2 + f, : 2 * SUBLANES] = jnp.where(inside, value, jnp.zeros_like(value))
        raw_out[f] = raw[f, 1 : 1 + SUBLANES] + bias[...].reshape(1, -1)
    sides = [edge_sides(edges, f) for f in range(2 + count)]
    parts = [edge_sums(sides[a : a + count], a, weight) for a in range(3)]
    for c in range(3):
        sums_out[c] = parts[0][c] + parts[1][c] + parts[2][c]


def near_kernel(*refs):
    left = lax.axis_index("wa") == 0
    out, start = refs[-1], 0
    for part in refs[:-1]:
        rows, cols = part.shape[1:3]
        out[:, start : start + rows] = jnp.where(left, part[:, :, cols - BLOCK :, :], part[:, :, :BLOCK, :])
        start += rows


def row_valid(count, rows, top, bottom, halo):
    row = lax.broadcasted_iota(jnp.int32, (count, 1), 0) % SUBLANES
    return jnp.logical_not((top & (row < halo)) | (bottom & (row >= rows - halo)))


def last_kernel(sib, weight, block_in, edge_in, sums_in, raw, folded, up_bias, done, out_hbm,
                near_prev, edges, wide, block, sent):
    left, core, top, bottom = place()
    count, mid, _, channels = block_in.shape
    rows = mid - 2
    cols = done.shape[2]
    rest = pl.ds(pl.multiple_of(core * BLOCK, BLOCK), cols - BLOCK)
    strip = pl.ds(pl.multiple_of((1 - core) * (cols - BLOCK), BLOCK), BLOCK)
    copies = [
        pltpu.make_async_copy(done.at[t, :, rest, :], out_hbm.at[t, :, rest, :], sent.at[t]) for t in range(count)
    ]
    for copy in copies:
        copy.start()
    unpack(sib[:, :HALO], near_prev, (1 - core) * HALO)
    unpack(sib[:, HALO:], near_prev, core * HALO)
    clear_outside(near_prev, top, bottom)
    edges[...] = jnp.zeros(edges.shape, jnp.float32)
    edge_columns(near_prev, (*range(HALO), *range(HALO + rows, rows + 2 * HALO)), edges, left)
    sides = [edge_sides(edges, f) for f in range(2)]
    parts = [edge_sums(sides[a : a + count], a, weight) for a in range(2)]
    inside = row_valid(SUBLANES, mid, top, bottom, 1)
    row = lax.broadcasted_iota(jnp.int32, (SUBLANES, 1), 0)
    blank = jnp.zeros((SUBLANES, channels), jnp.float32)
    inner, rim = [], []
    for t in range(count):
        span = slice(2 * SUBLANES * t, 2 * SUBLANES * (t + 1))
        sums = [functools.reduce(jnp.add, [part[c][span] for part in parts[: 2 - t]], sums_in[c, span]) for c in range(3)]
        near = [total[:SUBLANES] for total in sums]
        next_ = [total[SUBLANES:] for total in sums]
        edge = edge_in[t] + near[1] + jnp.where(left, next_[2], next_[0]) + raw[t]
        edges[t, :SUBLANES] = jnp.where(inside, edge, blank)
        rim.append(edges.at[t])
        lines = []
        for r in range(mid):
            change = jnp.where(left, near[2][r : r + 1], near[0][r : r + 1])
            value = block_in[t, r] + jnp.where(row == jnp.where(left, BLOCK - 1, 0), change, blank)
            if r in (0, mid - 1):
                value = jnp.where(bottom if r else top, blank, value)
            lines.append(value)
        inner.append(lines)
    windows = [
        jnp.concatenate(
            [value for lines in inner for value in lines[k : k + rows]] + [line[k : k + SUBLANES] for line in rim], axis=0
        ).astype(jnp.bfloat16)
        for k in range(3)
    ]
    line, early = phase_lines(up_bias, channels)
    nothing = jnp.zeros((1, channels), jnp.float32)
    fresh = (left & (row >= BLOCK - 2)) | (jnp.logical_not(left) & (row < 2))
    size = count * rows * BLOCK
    lo, hi = SUBLANES, SUBLANES + BLOCK
    for p in range(2):
        centre, sides = phase_sums(windows, folded, p)
        for t in range(count):
            for r in range(rows):
                at = t * rows + r
                value = sides[size + t * SUBLANES + r : size + t * SUBLANES + r + 1]
                wide[p, at, lo:hi, :] = sides[at * BLOCK : (at + 1) * BLOCK]
                wide[p, at, lo - 1 : lo, :] = jnp.where(left, nothing, value)
                wide[p, at, hi : hi + 1, :] = jnp.where(left, value, nothing)
                total = centre[at * BLOCK : (at + 1) * BLOCK] + line
                total = total + jnp.where(early, wide[p, at, lo - 1 : hi - 1, :], wide[p, at, lo + 1 : hi + 1, :])
                old = jnp.where(left, done[t, 2 * r + p, cols - BLOCK :, :], done[t, 2 * r + p, :BLOCK, :])
                block[t, 2 * r + p] = jnp.where(fresh, total, old.astype(jnp.float32)).astype(jnp.bfloat16)
    for t in range(count):
        copies.append(pltpu.make_async_copy(block.at[t], out_hbm.at[t, :, strip, :], sent.at[count + t]))
        copies[-1].start()
    for copy in copies:
        copy.wait()


VMEM = pl.BlockSpec(memory_space=pltpu.VMEM)
HBM = pl.BlockSpec(memory_space=pltpu.HBM)


def call(kernel, specs, shapes, scratch, flops, *args, outs=VMEM):
    return pl.pallas_call(
        kernel,
        out_shape=shapes,
        in_specs=specs,
        out_specs=jax.tree.map(lambda _: outs, shapes),
        scratch_shapes=scratch,
        cost_estimate=pl.CostEstimate(flops=flops, transcendentals=0, bytes_accessed=0),
        compiler_params=pltpu.CompilerParams(vmem_limit_bytes=16 * 1024 * 1024),
    )(*[pltpu.with_memory_space_constraint(arg, pltpu.HBM) if spec is HBM else arg for spec, arg in zip(specs, args)])


def block(frames, cache, norm_gain, conv_weight, conv_bias, up_weight, up_bias):
    count, rows, cols, channels = frames.shape
    outputs = up_weight.shape[-1]
    cores = lax.axis_size("wa")
    f32, bf16 = jnp.float32, jnp.bfloat16
    shape = jax.ShapeDtypeStruct
    part = shape((3, HALO, cols, LANES), bf16)
    sibling = [(i, cores - 1 - i) for i in range(cores)]
    along, against, later = snake((1, -1), 0), snake((-1, 1), 0), snake((1, -1), 1)
    first, second, raw_first, raw_second, act = call(
        pack_kernel, [HBM] * 3, (part, part, part, part, shape(frames.shape, bf16)),
        (pltpu.VMEM(frames.shape, bf16), pltpu.VMEM(cache.shape, bf16), pltpu.VMEM(norm_gain.shape, f32),
         pltpu.SemaphoreType.DMA((1 + 2 * count * rows,))),
        COST, frames, cache, norm_gain,
    )
    main_a = lax.ppermute(first, "ta", ring("ta"))
    main_b = lax.ppermute(second, "ta", ring("ta"))
    prev_a = lax.ppermute(second, AXES, later)
    own_a = lax.ppermute(raw_first, AXES, along)
    own_b = lax.ppermute(raw_second, AXES, against)
    prev_b = lax.ppermute(main_a, AXES, against)
    early = [main_a, main_b, own_a, own_b, raw_first, raw_second]
    sib_early = call(near_kernel, [VMEM] * 6, shape((3, 6 * HALO, BLOCK, LANES), bf16), (), 0, *early)
    sib_early = lax.ppermute(sib_early, "wa", sibling)
    sib = call(near_kernel, [VMEM] * 2, shape((3, 2 * HALO, BLOCK, LANES), bf16), (), 0, prev_a, prev_b)
    sib = lax.ppermute(sib, "wa", sibling)
    mid, all_rows = rows + 2, rows + 2 * HALO
    body_shape = shape((count, mid, cols, channels), f32)
    edge_shape = shape((count, SUBLANES, channels), f32)
    shift = pltpu.VMEM((mid, cols + 2 * SUBLANES, channels), f32)
    tile = pltpu.VMEM((2, rows, cols, channels), bf16)
    halo = pltpu.VMEM((2, 2 * HALO, cols, channels), bf16)
    body, edge = call(
        first_kernel, [VMEM] * 5, (body_shape, edge_shape), (tile, shift, shift),
        10**9, raw_first, raw_second, act, conv_weight, conv_bias,
    )
    body, edge = call(
        second_kernel, [VMEM] * 8, (body_shape, edge_shape), (tile, halo, halo, shift, shift),
        10**9, main_a, main_b, own_a, own_b, conv_weight, norm_gain, body, edge,
    )
    folded = call(fold_kernel, [VMEM], shape((8, channels, 2 * outputs), bf16), (), 3 * 10**9, up_weight)
    out_shape = (count, 2 * rows, cols, 2 * outputs)
    block, edge, out = call(
        third_kernel, [VMEM] * 7,
        (shape((count, mid, BLOCK, channels), f32), edge_shape, shape(out_shape, bf16)),
        (halo, shift, shift, pltpu.VMEM((count, mid, cols, channels), bf16),
         pltpu.VMEM((2, rows, cols + 2 * SUBLANES, channels), f32)), 10**9,
        prev_a, prev_b, conv_weight, folded, up_bias, body, edge,
    )
    sums, raw = call(
        edge_kernel, [VMEM] * 4, (shape((3, 2 * SUBLANES * count, channels), f32), edge_shape),
        (pltpu.VMEM((2, rows, BLOCK, channels), bf16), pltpu.VMEM((count, all_rows, BLOCK, channels), bf16),
         pltpu.VMEM((2 + count, 3 * SUBLANES, channels), f32), pltpu.VMEM((count, 3 * SUBLANES, channels), f32)),
        10**9, sib_early, conv_weight, norm_gain, conv_bias,
    )
    return call(
        last_kernel, [VMEM] * 9, shape(out_shape, bf16),
        (pltpu.VMEM((2, 2 * HALO, BLOCK, channels), bf16), pltpu.VMEM((2, 3 * SUBLANES, channels), f32),
         pltpu.VMEM((2, count * rows, BLOCK + 2 * SUBLANES, channels), f32),
         pltpu.VMEM((count, 2 * rows, BLOCK, 2 * outputs), bf16), pltpu.SemaphoreType.DMA((2 * count,))),
        10**9, sib, conv_weight, block, edge, sums, raw, folded, up_bias, out, outs=HBM,
    )


def solution(mesh):
    return jax.shard_map(
        block,
        mesh=mesh,
        in_specs=(
            P(("clips", "ta"), "ha", "wa", None),
            P("clips", "ha", "wa", None),
            P(),
            P(),
            P(),
            P(),
            P(),
        ),
        out_specs=P(("clips", "ta"), "ha", "wa", None),
        check_vma=False,
    )
```
